32 devices in a mesh: batch: 2 (over x), ysp: 4 (over z), xsp: 4 (over y, core).
Axes of the slice: x: 2, y: 2, z: 4, core: 2. Of those that a mesh axis runs over, the one named last changes fastest.
Arguments:
- volume: bfloat16 [640, 96, 96, 64], P('batch', 'xsp', 'ysp'), parts along dimension 0
- filter_taps: float32 [3, 3, 15], replicated
- mix_weights: bfloat16 [3, 320, 320], replicated
- mix_bias: float32 [3, 320], replicated
Outputs:
- output: bfloat16 [640, 96, 96, 64], P('batch', 'xsp', 'ysp'), parts along dimension 0
There are 2 independent parts. The reference program is written for one: setup_inputs(seed, part) draws one part's arguments, and reference() takes and returns one part's arrays. A program takes and returns all parts, laid end to end along the dimension named above; an argument that names none is the same for every part.
All inputs are finite; a program needn't handle non-finite values.
Results may differ from the reference program's by a relative error of at most 0.00554118.
Values are sent between devices in bfloat16 or wider.
A program may use at most 1 GiB of HBM per device.

```python
import jax
import jax.numpy as jnp
from jax import lax

CHANNELS = 320
FILTER_TAPS = 15
LAYERS = 3
GRID_X = 96
GRID_Y = 96
GRID_Z = 64
HALF_WIDTH = (FILTER_TAPS - 1) // 2


def setup_inputs(seed: int = 0, part: int = 0) -> dict:
    vol_key = jax.random.fold_in(jax.random.key(seed), part)
    key_sign, key_mag, key_mix, key_bias = jax.random.split(jax.random.key(seed + 1), 4)
    volume = jax.random.normal(vol_key, (CHANNELS, GRID_X, GRID_Y, GRID_Z), jnp.float32)
    tap_signs = jnp.where(jax.random.bernoulli(key_sign, 0.5, (LAYERS, 3, FILTER_TAPS)), 1.0, -1.0)
    tap_mags = jax.random.uniform(key_mag, (LAYERS, 3, FILTER_TAPS), jnp.float32, 0.5, 1.0)
    raw_taps = tap_signs * tap_mags
    filter_taps = raw_taps / jnp.sqrt(jnp.sum(raw_taps * raw_taps, axis=-1, keepdims=True))
    mix_weights = jax.random.normal(key_mix, (LAYERS, CHANNELS, CHANNELS), jnp.float32) * CHANNELS ** -0.5
    mix_bias = 0.5 * jax.random.normal(key_bias, (LAYERS, CHANNELS), jnp.float32)
    return {"volume": volume.astype(jnp.bfloat16), "filter_taps": filter_taps, "mix_weights": mix_weights.astype(jnp.bfloat16), "mix_bias": mix_bias}


def line_filter(channel_vol, tap_row, dim_index):
    extent = channel_vol.shape[dim_index]
    pad_cfg = [(0, 0), (0, 0), (0, 0)]
    pad_cfg[dim_index] = (HALF_WIDTH, HALF_WIDTH)
    padded = jnp.pad(channel_vol.astype(jnp.float32), pad_cfg)
    tap_vals = tap_row.astype(jnp.bfloat16).astype(jnp.float32)
    accum_sum = jnp.zeros(channel_vol.shape, jnp.float32)
    for tap_pos in range(FILTER_TAPS):
        accum_sum = accum_sum + tap_vals[tap_pos] * lax.slice_in_dim(padded, tap_pos, tap_pos + extent, axis=dim_index)
    return accum_sum.astype(jnp.bfloat16)


def reference(volume, filter_taps, mix_weights, mix_bias):
    def layer_step(current, params):
        tap_set, mix_mat, bias_vec = params

        def filter_channel(channel_vol):
            x_filtered = line_filter(channel_vol, tap_set[0], 0)
            xy_filtered = line_filter(x_filtered, tap_set[1], 1)
            return line_filter(xy_filtered, tap_set[2], 2)

        smooth = lax.map(filter_channel, current)
        mix_f32 = mix_mat.astype(jnp.float32)

        def mix_plane(pair):
            plane_u, plane_v = pair
            pre_act = jnp.einsum("cd,cyz->dyz", mix_f32, plane_u.astype(jnp.float32)) + bias_vec[:, None, None]
            return (plane_v.astype(jnp.float32) + jax.nn.gelu(pre_act, approximate=True)).astype(jnp.bfloat16)

        planes = lax.map(mix_plane, (jnp.moveaxis(smooth, 1, 0), jnp.moveaxis(current, 1, 0)))
        return jnp.moveaxis(planes, 0, 1), None

    result, _ = lax.scan(layer_step, volume, (filter_taps, mix_weights, mix_bias))
    return result
```

```python
import functools

import jax
import jax.numpy as jnp
from jax import lax
from jax.experimental import pallas as pl
from jax.experimental.pallas import tpu as pltpu
from jax.sharding import PartitionSpec as P

PARTS_AXIS = "batch"
COL_AXIS = "ysp"
ROW_AXIS = "xsp"
BF = jnp.bfloat16
F32 = jnp.float32
ZB = 16


class Dims:
    def __init__(self, shape, taps):
        self.c, self.nx, self.ny, self.nz = shape
        self.h = (taps - 1) // 2
        self.taps = taps
        self.cm = 256
        self.cr = self.c - self.cm
        self.rep = self.cm // self.cr
        self.rows = self.nz + self.nz // self.rep
        self.slabs = self.rows // ZB
        self.mid = self.nx - 2 * self.h


def params(flops=0, nbytes=0, vmem=None):
    return dict(
        cost_estimate=pl.CostEstimate(flops=int(flops), bytes_accessed=int(nbytes), transcendentals=0),
        compiler_params=pltpu.CompilerParams(vmem_limit_bytes=vmem or 60 * 2**20),
    )


def build_kernel(d, taps_ref, band_ref, zband_ref):
    n_layers = zband_ref.shape[0]
    rows, cols = band_ref.shape[2:]
    r = lax.broadcasted_iota(jnp.int32, (rows, cols), 0)
    s = lax.broadcasted_iota(jnp.int32, (rows, cols), 1)
    diff = jnp.where((r & (ZB - 1)) == (s & (ZB - 1)), s // ZB - r // ZB, -1)
    zr = lax.broadcasted_iota(jnp.int32, (d.nz, d.nz), 0)
    zs = lax.broadcasted_iota(jnp.int32, (d.nz, d.nz), 1)
    zdiff = zs - zr + d.h
    for layer in range(n_layers):
        for axis in range(2):
            acc = jnp.zeros((rows, cols), F32)
            for t in range(d.taps):
                acc = jnp.where(diff == t, taps_ref[layer * 3 + axis, t], acc)
            band_ref[layer, axis] = acc.astype(BF)
        acc = jnp.zeros((d.nz, d.nz), F32)
        for t in range(d.taps):
            acc = jnp.where(zdiff == t, taps_ref[layer * 3 + 2, t], acc)
        zband_ref[layer] = acc.astype(BF)


def build_bands(d, taps):
    n_layers = taps.shape[0]
    return pl.pallas_call(
        functools.partial(build_kernel, d),
        out_shape=(
            jax.ShapeDtypeStruct((n_layers, 2, d.mid * ZB, d.nx * ZB), BF),
            jax.ShapeDtypeStruct((n_layers, d.nz, d.nz), BF),
        ),
        in_specs=[pl.BlockSpec(memory_space=pltpu.SMEM)],
        out_specs=(pl.BlockSpec(memory_space=pltpu.VMEM), pl.BlockSpec(memory_space=pltpu.VMEM)),
        name="bands",
        **params(1e6, 1e6),
    )(taps.reshape(n_layers * 3, d.taps))


def lane_block(d, n_rows):
    return lax.broadcasted_iota(jnp.int32, (n_rows, d.cm), 1) // d.cr


def pack_rest(d, spread):
    step = d.nz // d.rep
    blk = lane_block(d, step)
    out = spread[0:step]
    for q in range(1, d.rep):
        out = jnp.where(blk == q, spread[q * step:(q + 1) * step], out)
    return out


def pack_kernel(d, v_ref, o_ref):
    m = lax.broadcasted_iota(jnp.int32, (d.cr, d.cm), 0)
    n = lax.broadcasted_iota(jnp.int32, (d.cr, d.cm), 1)
    spread_mat = jnp.where(n % d.cr == m, 1.0, 0.0).astype(BF)

    def body(y, carry):
        o_ref[0, y, 0:d.nz, :] = v_ref[0, y, :, 0:d.cm]
        rest = v_ref[0, y, :, d.cm:d.c]
        spread = jnp.dot(rest, spread_mat, preferred_element_type=F32)
        o_ref[0, y, d.nz:d.rows, :] = pack_rest(d, spread).astype(BF)
        return carry

    lax.fori_loop(0, d.ny, body, 0, unroll=4)


def pack(d, vol, x0, n):
    return pl.pallas_call(
        functools.partial(pack_kernel, d),
        grid=(n,),
        out_shape=jax.ShapeDtypeStruct((n, d.ny, d.rows, d.cm), BF),
        in_specs=[pl.BlockSpec((1, d.ny, d.nz, d.c), lambda i: (x0 + i, 0, 0, 0))],
        out_specs=pl.BlockSpec((1, d.ny, d.rows, d.cm), lambda i: (i, 0, 0, 0)),
        name="pack",
        **params(n * 1e7, n * 2.2e6),
    )(vol)


def xfilt_kernel(d, n_out, n_cols, *refs):
    t_ref = refs[0]
    ins = refs[1:1 + 3 * n_cols]
    outs = refs[1 + 3 * n_cols:]
    t_mat = t_ref[...]
    for col in range(n_cols):
        trio = ins[3 * col:3 * col + 3]
        for s in range(d.slabs):
            sl = slice(s * ZB, (s + 1) * ZB)
            rhs = jnp.concatenate([r[:, 0, sl, :].reshape(r.shape[0] * ZB, d.cm) for r in trio], axis=0)
            res = jnp.dot(t_mat, rhs, preferred_element_type=F32).astype(BF).reshape(n_out, ZB, d.cm)
            outs[col][:, 0, sl, :] = res


def xfilt(d, t_mat, trio, ys, steps):
    n_out = t_mat.shape[0] // ZB
    n_cols = len(ys)
    in_specs = [pl.BlockSpec(t_mat.shape, lambda i: (0, 0))]
    args = [t_mat]
    for y_of in ys:
        for a in trio:
            in_specs.append(pl.BlockSpec((a.shape[0], 1, d.rows, d.cm), lambda i, f=y_of: (0, f(i), 0, 0)))
            args.append(a)
    out = jax.ShapeDtypeStruct((n_out, steps, d.rows, d.cm), BF)
    return pl.pallas_call(
        functools.partial(xfilt_kernel, d, n_out, n_cols),
        grid=(steps,),
        out_shape=[out] * n_cols,
        in_specs=in_specs,
        out_specs=[pl.BlockSpec((n_out, 1, d.rows, d.cm), lambda i: (0, i, 0, 0))] * n_cols,
        name="xfilt",
        **params(2 * steps * n_cols * d.slabs * t_mat.shape[0] * 384 * 256, steps * n_cols * 34 * 40960),
    )(*args)


def gelu(x):
    return x * (0.5 * (1.0 + jnp.tanh(0.7978845608028654 * (x + 0.044715 * (x * x * x)))))


def tail_kernel(d, group, last, t_ref, z_ref, wm_ref, wr_ref, b_ref, hl, lo, mi, hi, hr, v_ref, o_ref, um_ref, ur_ref):
    h, step = d.h, d.nz // d.rep
    parts = (
        (0, h, slice(0, h * ZB), (hl, lo, mi)),
        (h, d.mid, slice(0, d.mid * ZB), (lo, mi, hi)),
        (h + d.mid, h, slice((d.mid - h) * ZB, d.mid * ZB), (mi, hi, hr)),
    )
    for y0, n, rows, trio in parts:
        t_mat = t_ref[rows, :]
        for s in range(d.slabs):
            sl = slice(s * ZB, (s + 1) * ZB)
            rhs = jnp.concatenate([r[0, :, sl, :].reshape(r.shape[1] * ZB, d.cm) for r in trio], axis=0)
            res = jnp.dot(t_mat, rhs, preferred_element_type=F32)
            if s * ZB < d.nz:
                um_ref[y0:y0 + n, sl, :] = res.astype(BF).reshape(n, ZB, d.cm)
            else:
                r0 = s * ZB - d.nz
                for q in range(d.rep):
                    piece = res[:, q * d.cr:(q + 1) * d.cr].astype(BF).reshape(n, ZB, d.cr)
                    ur_ref[y0:y0 + n, q * step + r0:q * step + r0 + ZB, :] = piece
    z_mat = z_ref[...]
    b_main = b_ref[0:1, :]
    b_rest = b_ref[1:2, :]

    def body(g, carry):
        y0 = g * group
        mains, rests = [], []
        for k in range(group):
            mains.append(jnp.dot(z_mat, um_ref[y0 + k], preferred_element_type=F32).astype(BF))
            rests.append(jnp.dot(z_mat, ur_ref[y0 + k], preferred_element_type=F32).astype(BF))
        um = jnp.concatenate(mains, axis=0)
        ur = jnp.concatenate(rests, axis=0)
        main = jnp.dot(um, wm_ref[:, 0:d.cm], preferred_element_type=F32) + jnp.dot(ur, wr_ref[:, 0:d.cm], preferred_element_type=F32)
        rest = jnp.dot(um, wm_ref[:, d.cm:], preferred_element_type=F32) + jnp.dot(ur, wr_ref[:, d.cm:], preferred_element_type=F32)
        for k in range(group):
            m = gelu(main[k * d.nz:(k + 1) * d.nz] + b_main) + v_ref[0, y0 + k, 0:d.nz, :].astype(F32)
            r = gelu(pack_rest(d, rest[k * d.nz:(k + 1) * d.nz]) + b_rest) + v_ref[0, y0 + k, d.nz:d.rows, :].astype(F32)
            if last:
                o_ref[0, y0 + k, :, 0:d.cm] = m.astype(BF)
                for q in range(d.rep):
                    o_ref[0, y0 + k, q * step:(q + 1) * step, d.cm:d.c] = r[:, q * d.cr:(q + 1) * d.cr].astype(BF)
            else:
                o_ref[0, y0 + k, 0:d.nz, :] = m.astype(BF)
                o_ref[0, y0 + k, d.nz:d.rows, :] = r.astype(BF)
        return carry

    lax.fori_loop(0, d.ny // group, body, 0)


def tail(d, t_mat, z_mat, wm, wr, bias, us, v, group=4, out_buf=None, x0=0, last=False):
    n = v.shape[0]
    consts = [t_mat, z_mat, wm, wr, bias]
    in_specs = [pl.BlockSpec(a.shape, lambda i: (0, 0)) for a in consts]
    for a in list(us) + [v]:
        in_specs.append(pl.BlockSpec((1,) + a.shape[1:], lambda i: (i, 0, 0, 0)))
    args = consts + list(us) + [v]
    alias = {}
    kern = functools.partial(tail_kernel, d, group, last)
    if last:
        out_shape = jax.ShapeDtypeStruct((d.nx, d.ny, d.nz, d.c), BF)
        out_spec = pl.BlockSpec((1, d.ny, d.nz, d.c), lambda i: (x0 + i, 0, 0, 0))
        if out_buf is not None:
            alias = {len(args): 0}
            args = args + [out_buf]
            in_specs.append(pl.BlockSpec(memory_space=pl.ANY))
            base = kern
            kern = lambda *r: base(*r[:11], *r[12:])
    else:
        out_shape = jax.ShapeDtypeStruct((n, d.ny, d.rows, d.cm), BF)
        out_spec = pl.BlockSpec((1, d.ny, d.rows, d.cm), lambda i: (i, 0, 0, 0))
    return pl.pallas_call(
        kern,
        grid=(n,),
        out_shape=out_shape,
        in_specs=in_specs,
        out_specs=out_spec,
        scratch_shapes=[pltpu.VMEM((d.ny, d.nz, d.cm), BF), pltpu.VMEM((d.ny, d.nz, d.cr), BF)],
        input_output_aliases=alias,
        name="tail",
        **params(2 * n * d.ny * 544 * 256 * 256, n * 3.6e6),
    )(*args)


def solution(mesh):
    x_count = mesh.shape[ROW_AXIS]
    y_count = mesh.shape[COL_AXIS]
    vol_spec = P(PARTS_AXIS, ROW_AXIS, COL_AXIS, None)

    def up(a, axis, n):
        return lax.ppermute(a, axis, [(s, s + 1) for s in range(n - 1)])

    def down(a, axis, n):
        return lax.ppermute(a, axis, [(s + 1, s) for s in range(n - 1)])

    def local_layers(volume, filter_taps, mix_weights, mix_bias):
        n_layers = filter_taps.shape[0]
        d = Dims(volume.shape, filter_taps.shape[-1])
        h, mid = d.h, d.mid
        vol = jnp.transpose(volume, (1, 2, 3, 0))
        band, zband = build_bands(d, filter_taps)
        w_ext = jnp.concatenate([mix_weights[:, :, :d.cm]] + [mix_weights[:, :, d.cm:]] * d.rep, axis=2)
        wm, wr = w_ext[:, :d.cm], w_ext[:, d.cm:]
        bias = jnp.stack([mix_bias[:, :d.cm], jnp.concatenate([mix_bias[:, d.cm:]] * d.rep, axis=1)], axis=1)
        v = {"P": pack(d, vol, 0, h), "R": pack(d, vol, h + mid, h), "Q": pack(d, vol, h, mid)}
        out = None
        for layer in range(n_layers):
            tx, ty, tz = band[layer, 0], band[layer, 1], zband[layer]
            from_left = up(v["R"], ROW_AXIS, x_count)
            from_right = down(v["P"], ROW_AXIS, x_count)
            spec = {
                "Q": (tx, (v["P"], v["Q"], v["R"])),
                "P": (tx[0:h * ZB], (from_left, v["P"], v["Q"])),
                "R": (tx[(mid - h) * ZB:], (v["Q"], v["R"], from_right)),
            }
            order = "QPR" if layer % 2 == 0 else "QRP"
            last = layer == n_layers - 1
            us = {}
            for ch in order:
                t_mat, trio = spec[ch]
                lo, hi = xfilt(d, t_mat, trio, [lambda i: i, lambda i: h + mid + i], h)
                hl = up(hi, COL_AXIS, y_count)
                hr = down(lo, COL_AXIS, y_count)
                (mi,) = xfilt(d, t_mat, trio, [lambda i: h + i], mid)
                us[ch] = (hl, lo, mi, hi, hr)
            new_v = {}
            for ch in order:
                x0 = {"P": 0, "Q": h, "R": h + mid}[ch]
                res = tail(d, ty, tz, wm[layer], wr[layer], bias[layer], us[ch], v[ch], out_buf=out, x0=x0, last=last)
                if last:
                    out = res
                else:
                    new_v[ch] = res
            v = new_v
        return jnp.transpose(out, (3, 0, 1, 2))

    return jax.shard_map(local_layers, mesh=mesh, in_specs=(vol_spec, P(), P(), P()), out_specs=vol_spec, check_vma=False)
```

```python
import functools

import jax
import jax.numpy as jnp
from jax import lax
from jax.experimental import pallas as pl
from jax.experimental.pallas import tpu as pltpu
from jax.sharding import PartitionSpec as P


PARTS_AXIS = "batch"
COL_AXIS = "ysp"
ROW_AXIS = "xsp"
BF = jnp.bfloat16
F32 = jnp.float32
ZB = 16
VMEM_BYTES = 67043328


class Dims:
    def __init__(self, shape, taps):
        self.c, self.nx, self.ny, self.nz = shape
        self.h = (taps - 1) // 2
        self.taps = taps
        self.cm = 256
        self.cr = self.c - self.cm
        self.rep = self.cm // self.cr
        self.rows = self.nz + self.nz // self.rep
        self.slabs = self.rows // ZB
        self.mid = self.nx - 2 * self.h


def params(nbytes):
    return dict(
        cost_estimate=pl.CostEstimate(flops=0, bytes_accessed=int(nbytes), transcendentals=0),
        compiler_params=pltpu.CompilerParams(vmem_limit_bytes=VMEM_BYTES),
    )


def banded(d, taps_ref, row, out_of, in_of, n_out):
    shape = (n_out * ZB, (2 * d.h + d.mid) * ZB)
    r = lax.broadcasted_iota(jnp.int32, shape, 0)
    s = lax.broadcasted_iota(jnp.int32, shape, 1)
    diff = jnp.where((r & (ZB - 1)) == (s & (ZB - 1)), in_of(s // ZB) - out_of(r // ZB) + d.h, -1)
    acc = jnp.zeros(shape, F32)
    for t in range(d.taps):
        acc = jnp.where(diff == t, taps_ref[row, t], acc)
    return acc.astype(BF)


def build_kernel(d, taps_ref, inner_ref, mid_ref, outer_ref, y_ref, z_ref):
    h, mid, n = d.h, d.mid, d.nx
    for layer in range(z_ref.shape[0]):
        fx, fy, fz = 3 * layer, 3 * layer + 1, 3 * layer + 2
        inner_ref[layer] = banded(d, taps_ref, fx, lambda m: h + mid + m, lambda p: jnp.where(p < mid + h, h + p, 2 * n - 1 - p), h)
        mid_ref[layer] = banded(d, taps_ref, fx, lambda m: h + m, lambda p: p, mid)
        outer_ref[layer] = banded(d, taps_ref, fx, lambda m: m, lambda p: jnp.where(p < h, -1 - p, p - h), h)
        y_ref[layer] = banded(d, taps_ref, fy, lambda m: h + m, lambda p: p, mid)
        zr = lax.broadcasted_iota(jnp.int32, (d.nz, d.nz), 0)
        zs = lax.broadcasted_iota(jnp.int32, (d.nz, d.nz), 1)
        acc = jnp.zeros((d.nz, d.nz), F32)
        for t in range(d.taps):
            acc = jnp.where(zs - zr + d.h == t, taps_ref[fz, t], acc)
        z_ref[layer] = acc.astype(BF)


def build_bands(d, taps):
    n_layers = taps.shape[0]
    cols = (2 * d.h + d.mid) * ZB
    shapes = [(d.h * ZB, cols), (d.mid * ZB, cols), (d.h * ZB, cols), (d.mid * ZB, cols), (d.nz, d.nz)]
    return pl.pallas_call(
        functools.partial(build_kernel, d),
        out_shape=[jax.ShapeDtypeStruct((n_layers,) + s, BF) for s in shapes],
        in_specs=[pl.BlockSpec(memory_space=pltpu.SMEM)],
        out_specs=[pl.BlockSpec(memory_space=pltpu.VMEM)] * len(shapes),
        name="bands",
        **params(1e6),
    )(taps.reshape(n_layers * 3, d.taps))


def lane_block(d, n_rows):
    return lax.broadcasted_iota(jnp.int32, (n_rows, d.cm), 1) // d.cr


def pack_rest(d, spread):
    step = d.nz // d.rep
    blk = lane_block(d, step)
    out = spread[0:step]
    for q in range(1, d.rep):
        out = jnp.where(blk == q, spread[q * step:(q + 1) * step], out)
    return out


def pack_kernel(d, flip_ref, v_ref, dep_ref, o_ref):
    m = lax.broadcasted_iota(jnp.int32, (d.cr, d.cm), 0)
    n = lax.broadcasted_iota(jnp.int32, (d.cr, d.cm), 1)
    spread_mat = jnp.where(n % d.cr == m, 1.0, 0.0).astype(BF)
    for y in range(d.ny):
        o_ref[0, y, 0:d.nz, :] = v_ref[0, y, :, 0:d.cm]
        rest = v_ref[0, y, :, d.cm:d.c]
        spread = jnp.dot(rest, spread_mat, preferred_element_type=F32)
        o_ref[0, y, d.nz:d.rows, :] = pack_rest(d, spread).astype(BF)


def mirrored(d, u, flip):
    return u + flip * (d.nx - 1 - 2 * u)


def pack(d, dep, flip, vol, u0, n):
    return pl.pallas_call(
        functools.partial(pack_kernel, d),
        out_shape=jax.ShapeDtypeStruct((n, d.ny, d.rows, d.cm), BF),
        grid_spec=pltpu.PrefetchScalarGridSpec(
            num_scalar_prefetch=1,
            grid=(n,),
            in_specs=[
                pl.BlockSpec((1, d.ny, d.nz, d.c), lambda i, f: (mirrored(d, u0 + i, f[0]), 0, 0, 0)),
                pl.BlockSpec(memory_space=pl.ANY),
            ],
            out_specs=pl.BlockSpec((1, d.ny, d.rows, d.cm), lambda i, f: (i, 0, 0, 0)),
        ),
        name="pack",
        **params(n * 2.2e6),
    )(flip, vol, dep)


def xfilt_kernel(d, jobs, n_ins, n_mats, *refs):
    mats = [r[...] for r in refs[:n_mats]]
    ins = refs[n_mats:n_mats + n_ins]
    outs = refs[n_mats + n_ins + 1:]
    for out, (mat, planes) in zip(outs, jobs):
        n_out = out.shape[0]
        for s in range(d.slabs):
            sl = slice(s * ZB, (s + 1) * ZB)
            rhs = jnp.concatenate([ins[p][:, 0, sl, :].reshape(ins[p].shape[0] * ZB, d.cm) for p in planes], axis=0)
            res = jnp.dot(mats[mat], rhs, preferred_element_type=F32)
            out[:, 0, sl, :] = res.astype(BF).reshape(n_out, ZB, d.cm)


def xfilt(d, dep, mats, ins, jobs, steps):
    in_specs = [pl.BlockSpec(m.shape, lambda i: (0, 0)) for m in mats]
    for a, y_of in ins:
        in_specs.append(pl.BlockSpec((a.shape[0], 1, d.rows, d.cm), lambda i, f=y_of: (0, f(i), 0, 0)))
    in_specs.append(pl.BlockSpec(memory_space=pl.ANY))
    n_outs = [mats[m].shape[0] // ZB for m, _ in jobs]
    moved = sum(a.shape[0] for a, _ in ins) + sum(n_outs)
    return pl.pallas_call(
        functools.partial(xfilt_kernel, d, jobs, len(ins), len(mats)),
        grid=(steps,),
        out_shape=[jax.ShapeDtypeStruct((n, steps, d.rows, d.cm), BF) for n in n_outs],
        in_specs=in_specs,
        out_specs=[pl.BlockSpec((n, 1, d.rows, d.cm), lambda i: (0, i, 0, 0)) for n in n_outs],
        name="xfilt",
        **params(steps * moved * 40960),
    )(*mats, *[a for a, _ in ins], dep)


def xfilt_edges(d, dep, mat, trio):
    ins = [(a, lambda i: i) for a in trio] + [(a, lambda i: d.h + d.mid + i) for a in trio]
    return xfilt(d, dep, [mat], ins, [(0, (0, 1, 2)), (0, (3, 4, 5))], d.h)


def gelu(x):
    return x * (0.5 * (1.0 + jnp.tanh(0.7978845608028654 * (x + 0.044715 * (x * x * x)))))


def tail_kernel(d, last, flip_ref, t_ref, z_ref, wm_ref, wr_ref, b_ref, hl, lo, mi, hi, hr, v_ref, dep_ref, *rest_refs):
    o_ref, um_ref, ur_ref = rest_refs[-3:]
    h, step = d.h, d.nz // d.rep
    parts = (
        (0, h, slice(0, h * ZB), (hl, lo, mi)),
        (h, d.mid, slice(0, d.mid * ZB), (lo, mi, hi)),
        (h + d.mid, h, slice((d.mid - h) * ZB, d.mid * ZB), (mi, hi, hr)),
    )
    z_mat = z_ref[...]
    b_main = b_ref[0:1, :]
    b_rest = b_ref[1:2, :]
    for y0, n, rows, trio in parts:
        t_mat = t_ref[rows, :]
        for s in range(d.slabs):
            sl = slice(s * ZB, (s + 1) * ZB)
            rhs = jnp.concatenate([r[0, :, sl, :].reshape(r.shape[1] * ZB, d.cm) for r in trio], axis=0)
            res = jnp.dot(t_mat, rhs, preferred_element_type=F32)
            if s * ZB < d.nz:
                um_ref[y0:y0 + n, sl, :] = res.astype(BF).reshape(n, ZB, d.cm)
            else:
                r0 = s * ZB - d.nz
                for q in range(d.rep):
                    piece = res[:, q * d.cr:(q + 1) * d.cr].astype(BF).reshape(n, ZB, d.cr)
                    ur_ref[y0:y0 + n, q * step + r0:q * step + r0 + ZB, :] = piece
    mains, rests = [], []
    for y in range(d.ny):
        mains.append(jnp.dot(z_mat, um_ref[y], preferred_element_type=F32).astype(BF))
        rests.append(jnp.dot(z_mat, ur_ref[y], preferred_element_type=F32).astype(BF))
    um = jnp.concatenate(mains, axis=0)
    ur = jnp.concatenate(rests, axis=0)
    main = jnp.dot(um, wm_ref[:, 0:d.cm], preferred_element_type=F32) + jnp.dot(ur, wr_ref[:, 0:d.cm], preferred_element_type=F32)
    rest = jnp.dot(um, wm_ref[:, d.cm:], preferred_element_type=F32) + jnp.dot(ur, wr_ref[:, d.cm:], preferred_element_type=F32)
    for y in range(d.ny):
        m = gelu(main[y * d.nz:(y + 1) * d.nz] + b_main) + v_ref[0, y, 0:d.nz, :].astype(F32)
        r = gelu(pack_rest(d, rest[y * d.nz:(y + 1) * d.nz]) + b_rest) + v_ref[0, y, d.nz:d.rows, :].astype(F32)
        if last:
            o_ref[0, y, :, 0:d.cm] = m.astype(BF)
            for q in range(d.rep):
                o_ref[0, y, q * step:(q + 1) * step, d.cm:d.c] = r[:, q * d.cr:(q + 1) * d.cr].astype(BF)
        else:
            o_ref[0, y, 0:d.nz, :] = m.astype(BF)
            o_ref[0, y, d.nz:d.rows, :] = r.astype(BF)


def tail(d, dep, flip, consts, us, v, last=False, u0=0, out_buf=None):
    n = v.shape[0]
    in_specs = [pl.BlockSpec(a.shape, lambda i, f: (0, 0)) for a in consts]
    for a in list(us) + [v]:
        in_specs.append(pl.BlockSpec((1,) + a.shape[1:], lambda i, f: (i, 0, 0, 0)))
    args = [flip] + list(consts) + list(us) + [v, dep]
    in_specs.append(pl.BlockSpec(memory_space=pl.ANY))
    alias = {}
    if last:
        out_shape = jax.ShapeDtypeStruct((d.nx, d.ny, d.nz, d.c), BF)
        out_spec = pl.BlockSpec((1, d.ny, d.nz, d.c), lambda i, f: (mirrored(d, u0 + i, f[0]), 0, 0, 0))
        if out_buf is not None:
            alias = {len(args): 0}
            args.append(out_buf)
            in_specs.append(pl.BlockSpec(memory_space=pl.ANY))
    else:
        out_shape = jax.ShapeDtypeStruct((n, d.ny, d.rows, d.cm), BF)
        out_spec = pl.BlockSpec((1, d.ny, d.rows, d.cm), lambda i, f: (i, 0, 0, 0))
    return pl.pallas_call(
        functools.partial(tail_kernel, d, last),
        out_shape=out_shape,
        grid_spec=pltpu.PrefetchScalarGridSpec(
            num_scalar_prefetch=1,
            grid=(n,),
            in_specs=in_specs,
            out_specs=out_spec,
            scratch_shapes=[pltpu.VMEM((d.ny, d.nz, d.cm), BF), pltpu.VMEM((d.ny, d.nz, d.cr), BF)],
        ),
        input_output_aliases=alias,
        name="tail",
        **params(n * 3.6e6),
    )(*args)


def solution(mesh):
    x_count = mesh.shape[ROW_AXIS]
    y_count = mesh.shape[COL_AXIS]
    vol_spec = P(PARTS_AXIS, ROW_AXIS, COL_AXIS, None)

    def swap(a, first):
        pairs = [(s, s + 1) for s in range(first, x_count - 1, 2)]
        return lax.ppermute(a, ROW_AXIS, pairs + [(b, a_) for a_, b in pairs])

    def share(lo, hi):
        below = lax.ppermute(hi, COL_AXIS, [(s, s + 1) for s in range(y_count - 1)])
        above = lax.ppermute(lo, COL_AXIS, [(s + 1, s) for s in range(y_count - 1)])
        return below, above

    def local_layers(volume, filter_taps, mix_weights, mix_bias):
        n_layers = filter_taps.shape[0]
        d = Dims(volume.shape, filter_taps.shape[-1])
        h, mid = d.h, d.mid
        middle = lambda i: h + i
        odd = lax.axis_index(ROW_AXIS) % 2
        flip = odd.astype(jnp.int32).reshape(1)
        taps = filter_taps.at[:, 0].set(jnp.where(odd == 1, filter_taps[:, 0, ::-1], filter_taps[:, 0]))
        vol = jnp.transpose(volume, (1, 2, 3, 0))
        w_ext = jnp.concatenate([mix_weights[:, :, :d.cm]] + [mix_weights[:, :, d.cm:]] * d.rep, axis=2)
        bias = jnp.stack([mix_bias[:, :d.cm], jnp.concatenate([mix_bias[:, d.cm:]] * d.rep, axis=1)], axis=1)
        v_in = pack(d, flip, flip, vol, h + mid, h)
        h_in = swap(v_in, 0)
        v_out = pack(d, v_in, flip, vol, 0, h)
        h_out = swap(v_out, 1)
        v_mid = pack(d, v_out, flip, vol, h, mid)
        t_in, t_mid, t_out, t_y, t_z = build_bands(d, taps)
        lo_in, hi_in = xfilt_edges(d, v_mid, t_in[0], (v_mid, v_in, h_in))
        s_in = share(lo_in, hi_in)
        dep = lo_in
        res = None
        for layer in range(n_layers):
            last = layer == n_layers - 1
            consts = (t_y[layer], t_z[layer], w_ext[layer, :d.cm], w_ext[layer, d.cm:], bias[layer])
            if layer > 0:
                h_out = swap(v_out, 1)
            lo_mid, hi_mid = xfilt_edges(d, dep, t_mid[layer], (v_out, v_mid, v_in))
            s_mid = share(lo_mid, hi_mid)
            m_mid, m_in = xfilt(
                d, lo_mid, [t_mid[layer], t_in[layer]],
                [(a, middle) for a in (v_out, v_mid, v_in, h_in)],
                [(0, (0, 1, 2)), (1, (1, 2, 3))], mid,
            )
            w_in = tail(d, m_mid, flip, consts, (s_in[0], lo_in, m_in, hi_in, s_in[1]), v_in, last, h + mid)
            if not last:
                h_in = swap(w_in, 0)
            dep = m_mid if last else w_in
            lo_out, hi_out = xfilt_edges(d, dep, t_out[layer], (h_out, v_out, v_mid))
            s_out = share(lo_out, hi_out)
            (m_out,) = xfilt(
                d, lo_out, [t_out[layer]],
                [(a, middle) for a in (h_out, v_out, v_mid)], [(0, (0, 1, 2))], mid,
            )
            w_mid = tail(d, m_out, flip, consts, (s_mid[0], lo_mid, m_mid, hi_mid, s_mid[1]), v_mid, last, h, w_in if last else None)
            us_out = (s_out[0], lo_out, m_out, hi_out, s_out[1])
            if last:
                res = tail(d, m_out, flip, consts, us_out, v_out, last, 0, w_mid)
                break
            lo_in, hi_in = xfilt_edges(d, w_mid, t_in[layer + 1], (w_mid, w_in, h_in))
            s_in = share(lo_in, hi_in)
            w_out = tail(d, lo_in, flip, consts, us_out, v_out)
            v_in, v_mid, v_out = w_in, w_mid, w_out
            dep = w_out
        return jnp.transpose(res, (3, 0, 1, 2))

    return jax.shard_map(local_layers, mesh=mesh, in_specs=(vol_spec, P(), P(), P()), out_specs=vol_spec, check_vma=False)
```

```python
import functools

import jax
import jax.numpy as jnp
from jax import lax
from jax.experimental import pallas as pl
from jax.experimental.pallas import tpu as pltpu
from jax.sharding import PartitionSpec as P


PARTS_AXIS = "batch"
COL_AXIS = "ysp"
ROW_AXIS = "xsp"
BF = jnp.bfloat16
F32 = jnp.float32
ZB = 16
VMEM_BYTES = 67043328


class Dims:
    def __init__(self, shape, taps):
        self.c, self.nx, self.ny, self.nz = shape
        self.h = (taps - 1) // 2
        self.taps = taps
        self.cm = 256
        self.cr = self.c - self.cm
        self.rep = self.cm // self.cr
        self.rows = self.nz + self.nz // self.rep
        self.slabs = self.rows // ZB
        self.mid = self.nx - 2 * self.h


def params(nbytes):
    return dict(
        cost_estimate=pl.CostEstimate(flops=0, bytes_accessed=int(nbytes), transcendentals=0),
        compiler_params=pltpu.CompilerParams(vmem_limit_bytes=VMEM_BYTES),
    )


def banded(d, tap_of, out_of, in_of, n_out):
    shape = (n_out * ZB, (2 * d.h + d.mid) * ZB)
    r = lax.broadcasted_iota(jnp.int32, shape, 0)
    s = lax.broadcasted_iota(jnp.int32, shape, 1)
    diff = jnp.where((r & (ZB - 1)) == (s & (ZB - 1)), in_of(s // ZB) - out_of(r // ZB) + d.h, -1)
    acc = jnp.zeros(shape, F32)
    for t in range(d.taps):
        acc = jnp.where(diff == t, tap_of(t), acc)
    return acc.astype(BF)


def x_taps(d, flip_ref, taps_ref, layer):
    flip = flip_ref[0]
    return lambda t: taps_ref[layer, 0, t + flip * (d.taps - 1 - 2 * t)]


def first_kernel(d, flip_ref, taps_ref, o_ref):
    o_ref[...] = banded(d, x_taps(d, flip_ref, taps_ref, 0), lambda m: d.h + m, lambda p: mirrored(d, p, flip_ref[0]), d.mid)


def build_kernel(d, flip_ref, taps_ref, dep_ref, inner_ref, mid_ref, outer_ref, y_ref, z_ref):
    h, mid, n = d.h, d.mid, d.nx
    for layer in range(z_ref.shape[0]):
        tap_x = x_taps(d, flip_ref, taps_ref, layer)
        inner_ref[layer] = banded(d, tap_x, lambda m: h + mid + m, lambda p: jnp.where(p < mid + h, h + p, 2 * n - 1 - p), h)
        mid_ref[layer] = banded(d, tap_x, lambda m: h + m, lambda p: p, mid)
        outer_ref[layer] = banded(d, tap_x, lambda m: m, lambda p: jnp.where(p < h, -1 - p, p - h), h)
        y_ref[layer] = banded(d, lambda t: taps_ref[layer, 1, t], lambda m: h + m, lambda p: p, mid)
        zr = lax.broadcasted_iota(jnp.int32, (d.nz, d.nz), 0)
        zs = lax.broadcasted_iota(jnp.int32, (d.nz, d.nz), 1)
        acc = jnp.zeros((d.nz, d.nz), F32)
        for t in range(d.taps):
            acc = jnp.where(zs - zr + d.h == t, taps_ref[layer, 2, t], acc)
        z_ref[layer] = acc.astype(BF)


def build_first(d, flip, taps):
    return pl.pallas_call(
        functools.partial(first_kernel, d),
        out_shape=jax.ShapeDtypeStruct((d.mid * ZB, (2 * d.h + d.mid) * ZB), BF),
        in_specs=[pl.BlockSpec(memory_space=pltpu.SMEM)] * 2,
        out_specs=pl.BlockSpec(memory_space=pltpu.VMEM),
        name="band_first",
        **params(2e5),
    )(flip, taps)


def build_bands(d, dep, flip, taps):
    n_layers = taps.shape[0]
    cols = (2 * d.h + d.mid) * ZB
    shapes = [(d.h * ZB, cols), (d.mid * ZB, cols), (d.h * ZB, cols), (d.mid * ZB, cols), (d.nz, d.nz)]
    return pl.pallas_call(
        functools.partial(build_kernel, d),
        out_shape=[jax.ShapeDtypeStruct((n_layers,) + s, BF) for s in shapes],
        in_specs=[pl.BlockSpec(memory_space=pltpu.SMEM)] * 2 + [pl.BlockSpec(memory_space=pl.ANY)],
        out_specs=[pl.BlockSpec(memory_space=pltpu.VMEM)] * len(shapes),
        name="bands",
        **params(1e6),
    )(flip, taps, dep)


def lane_block(d, n_rows):
    return lax.broadcasted_iota(jnp.int32, (n_rows, d.cm), 1) // d.cr


def pack_rest(d, spread):
    step = d.nz // d.rep
    blk = lane_block(d, step)
    out = spread[0:step]
    for q in range(1, d.rep):
        out = jnp.where(blk == q, spread[q * step:(q + 1) * step], out)
    return out


def spread_matrix(d):
    m = lax.broadcasted_iota(jnp.int32, (d.cr, d.cm), 0)
    n = lax.broadcasted_iota(jnp.int32, (d.cr, d.cm), 1)
    return jnp.where(n % d.cr == m, 1.0, 0.0).astype(BF)


def place(d, refs, y):
    if len(refs) == 1:
        return refs[0], y
    if d.h <= y < d.h + d.mid:
        return refs[1], y - d.h
    return refs[0], y if y < d.h else y - d.mid


def chunk_shapes(d, n, split):
    return [(n, c, d.rows, d.cm) for c in ((2 * d.h, d.mid) if split else (d.ny,))]


def pack_kernel(d, flip_ref, v_ref, dep_ref, *o_refs):
    spread_mat = spread_matrix(d)
    for y in range(d.ny):
        o_ref, col = place(d, o_refs, y)
        o_ref[0, col, 0:d.nz, :] = v_ref[0, y, :, 0:d.cm]
        rest = v_ref[0, y, :, d.cm:d.c]
        spread = jnp.dot(rest, spread_mat, preferred_element_type=F32)
        o_ref[0, col, d.nz:d.rows, :] = pack_rest(d, spread).astype(BF)


def mirrored(d, u, flip):
    return u + flip * (d.nx - 1 - 2 * u)


def pack(d, dep, flip, vol, u0, n, split=False):
    shapes = chunk_shapes(d, n, split)
    return pl.pallas_call(
        functools.partial(pack_kernel, d),
        out_shape=[jax.ShapeDtypeStruct(s, BF) for s in shapes],
        grid_spec=pltpu.PrefetchScalarGridSpec(
            num_scalar_prefetch=1,
            grid=(n,),
            in_specs=[
                pl.BlockSpec((1, d.ny, d.nz, d.c), lambda i, f: (mirrored(d, u0 + i, f[0]), 0, 0, 0)),
                pl.BlockSpec(memory_space=pl.ANY),
            ],
            out_specs=[pl.BlockSpec((1,) + s[1:], lambda i, f: (i, 0, 0, 0)) for s in shapes],
        ),
        name="pack",
        **params(n * 2.2e6),
    )(flip, vol, dep)


def xfilt_kernel(d, jobs, n_ins, n_mats, *refs):
    mats = [r[...] for r in refs[:n_mats]]
    ins = refs[n_mats:n_mats + n_ins]
    outs = refs[n_mats + n_ins + 1:]
    for out, (mat, planes) in zip(outs, jobs):
        n_out = out.shape[0]
        for s in range(d.slabs):
            sl = slice(s * ZB, (s + 1) * ZB)
            rhs = jnp.concatenate([ins[p][:, 0, sl, :].reshape(ins[p].shape[0] * ZB, d.cm) for p in planes], axis=0)
            res = jnp.dot(mats[mat], rhs, preferred_element_type=F32)
            out[:, 0, sl, :] = res.astype(BF).reshape(n_out, ZB, d.cm)


def xfilt(d, dep, mats, ins, jobs, steps):
    in_specs = [pl.BlockSpec(m.shape, lambda i: (0, 0)) for m in mats]
    for a, y_of in ins:
        in_specs.append(pl.BlockSpec((a.shape[0], 1, d.rows, d.cm), lambda i, f=y_of: (0, f(i), 0, 0)))
    in_specs.append(pl.BlockSpec(memory_space=pl.ANY))
    n_outs = [mats[m].shape[0] // ZB for m, _ in jobs]
    moved = sum(a.shape[0] for a, _ in ins) + sum(n_outs)
    return pl.pallas_call(
        functools.partial(xfilt_kernel, d, jobs, len(ins), len(mats)),
        grid=(steps,),
        out_shape=[jax.ShapeDtypeStruct((n, steps, d.rows, d.cm), BF) for n in n_outs],
        in_specs=in_specs,
        out_specs=[pl.BlockSpec((n, 1, d.rows, d.cm), lambda i: (0, i, 0, 0)) for n in n_outs],
        name="xfilt",
        **params(steps * moved * 40960),
    )(*mats, *[a for a, _ in ins], dep)


def columns(d, v, part):
    if len(v) == 2:
        return {"lo": (v[0], lambda i: i), "hi": (v[0], lambda i: d.h + i), "mid": (v[1], lambda i: i)}[part]
    return v[0], {"lo": lambda i: i, "hi": lambda i: d.h + d.mid + i, "mid": lambda i: d.h + i}[part]


def xfilt_edges(d, dep, mat, trio):
    ins = [columns(d, v, "lo") for v in trio] + [columns(d, v, "hi") for v in trio]
    return xfilt(d, dep, [mat], ins, [(0, (0, 1, 2)), (0, (3, 4, 5))], d.h)


def xfilt_middle(d, dep, mats, vs, jobs):
    return xfilt(d, dep, mats, [columns(d, v, "mid") for v in vs], jobs, d.mid)


def direct_kernel(d, t_ref, lo_ref, hi_ref, lo_out, hi_out):
    spread_mat = spread_matrix(d)
    t_mat = t_ref[...]
    for v_ref, o_ref in ((lo_ref, lo_out), (hi_ref, hi_out)):
        rest = v_ref[:, 0, :, d.cm:d.c].reshape(d.nx * d.nz, d.cr)
        spread = jnp.dot(rest, spread_mat, preferred_element_type=F32)
        packed = [pack_rest(d, spread[p * d.nz:(p + 1) * d.nz]).astype(BF) for p in range(d.nx)]
        for s in range(d.slabs):
            sl = slice(s * ZB, (s + 1) * ZB)
            if s * ZB < d.nz:
                rhs = v_ref[:, 0, sl, 0:d.cm].reshape(d.nx * ZB, d.cm)
            else:
                r0 = s * ZB - d.nz
                rhs = jnp.concatenate([p[r0:r0 + ZB] for p in packed], axis=0)
            res = jnp.dot(t_mat, rhs, preferred_element_type=F32)
            o_ref[:, 0, sl, :] = res.astype(BF).reshape(d.mid, ZB, d.cm)


def direct_edges(d, mat, vol):
    block = (d.nx, 1, d.nz, d.c)
    out = jax.ShapeDtypeStruct((d.mid, d.h, d.rows, d.cm), BF)
    return pl.pallas_call(
        functools.partial(direct_kernel, d),
        grid=(d.h,),
        out_shape=[out, out],
        in_specs=[
            pl.BlockSpec(mat.shape, lambda i: (0, 0)),
            pl.BlockSpec(block, lambda i: (0, i, 0, 0)),
            pl.BlockSpec(block, lambda i: (0, d.h + d.mid + i, 0, 0)),
        ],
        out_specs=[pl.BlockSpec((d.mid, 1, d.rows, d.cm), lambda i: (0, i, 0, 0))] * 2,
        name="direct",
        **params(4e7),
    )(mat, vol, vol)


def gelu(x):
    return x * (0.5 * (1.0 + jnp.tanh(0.7978845608028654 * (x + 0.044715 * (x * x * x)))))


def tail_kernel(d, last, n_v, flip_ref, t_ref, z_ref, wm_ref, wr_ref, b_ref, hl, lo, mi, hi, hr, *more):
    v_refs = more[:n_v]
    um_ref, ur_ref = more[-2:]
    o_refs = more[-3:-2] if last else more[-2 - n_v:-2]
    h, step = d.h, d.nz // d.rep
    parts = (
        (0, h, slice(0, h * ZB), (hl, lo, mi)),
        (h, d.mid, slice(0, d.mid * ZB), (lo, mi, hi)),
        (h + d.mid, h, slice((d.mid - h) * ZB, d.mid * ZB), (mi, hi, hr)),
    )
    z_mat = z_ref[...]
    b_main = b_ref[0:1, :]
    b_rest = b_ref[1:2, :]
    for y0, n, rows, trio in parts:
        t_mat = t_ref[rows, :]
        for s in range(d.slabs):
            sl = slice(s * ZB, (s + 1) * ZB)
            rhs = jnp.concatenate([r[0, :, sl, :].reshape(r.shape[1] * ZB, d.cm) for r in trio], axis=0)
            res = jnp.dot(t_mat, rhs, preferred_element_type=F32)
            if s * ZB < d.nz:
                um_ref[y0:y0 + n, sl, :] = res.astype(BF).reshape(n, ZB, d.cm)
            else:
                r0 = s * ZB - d.nz
                for q in range(d.rep):
                    piece = res[:, q * d.cr:(q + 1) * d.cr].astype(BF).reshape(n, ZB, d.cr)
                    ur_ref[y0:y0 + n, q * step + r0:q * step + r0 + ZB, :] = piece
    mains, rests = [], []
    for y in range(d.ny):
        mains.append(jnp.dot(z_mat, um_ref[y], preferred_element_type=F32).astype(BF))
        rests.append(jnp.dot(z_mat, ur_ref[y], preferred_element_type=F32).astype(BF))
    um = jnp.concatenate(mains, axis=0)
    ur = jnp.concatenate(rests, axis=0)
    main = jnp.dot(um, wm_ref[:, 0:d.cm], preferred_element_type=F32) + jnp.dot(ur, wr_ref[:, 0:d.cm], preferred_element_type=F32)
    rest = jnp.dot(um, wm_ref[:, d.cm:], preferred_element_type=F32) + jnp.dot(ur, wr_ref[:, d.cm:], preferred_element_type=F32)
    for y in range(d.ny):
        v_ref, col = place(d, v_refs, y)
        m = gelu(main[y * d.nz:(y + 1) * d.nz] + b_main) + v_ref[0, col, 0:d.nz, :].astype(F32)
        r = gelu(pack_rest(d, rest[y * d.nz:(y + 1) * d.nz]) + b_rest) + v_ref[0, col, d.nz:d.rows, :].astype(F32)
        o_ref, col = place(d, o_refs, y)
        if last:
            o_ref[0, y, :, 0:d.cm] = m.astype(BF)
            for q in range(d.rep):
                o_ref[0, y, q * step:(q + 1) * step, d.cm:d.c] = r[:, q * d.cr:(q + 1) * d.cr].astype(BF)
        else:
            o_ref[0, col, 0:d.nz, :] = m.astype(BF)
            o_ref[0, col, d.nz:d.rows, :] = r.astype(BF)


def tail(d, dep, flip, consts, us, v, last=False, u0=0, out_buf=None):
    n = v[0].shape[0]
    blocks = list(us) + list(v)
    in_specs = [pl.BlockSpec(a.shape, lambda i, f: (0, 0)) for a in consts]
    in_specs += [pl.BlockSpec((1,) + a.shape[1:], lambda i, f: (i, 0, 0, 0)) for a in blocks]
    args = [flip] + list(consts) + blocks + [dep]
    in_specs.append(pl.BlockSpec(memory_space=pl.ANY))
    alias = {}
    if last:
        out_shape = [jax.ShapeDtypeStruct((d.nx, d.ny, d.nz, d.c), BF)]
        out_specs = [pl.BlockSpec((1, d.ny, d.nz, d.c), lambda i, f: (mirrored(d, u0 + i, f[0]), 0, 0, 0))]
        if out_buf is not None:
            alias = {len(args): 0}
            args.append(out_buf)
            in_specs.append(pl.BlockSpec(memory_space=pl.ANY))
    else:
        shapes = chunk_shapes(d, n, len(v) == 2)
        out_shape = [jax.ShapeDtypeStruct(s, BF) for s in shapes]
        out_specs = [pl.BlockSpec((1,) + s[1:], lambda i, f: (i, 0, 0, 0)) for s in shapes]
    return pl.pallas_call(
        functools.partial(tail_kernel, d, last, len(v)),
        out_shape=out_shape,
        grid_spec=pltpu.PrefetchScalarGridSpec(
            num_scalar_prefetch=1,
            grid=(n,),
            in_specs=in_specs,
            out_specs=out_specs,
            scratch_shapes=[pltpu.VMEM((d.ny, d.nz, d.cm), BF), pltpu.VMEM((d.ny, d.nz, d.cr), BF)],
        ),
        input_output_aliases=alias,
        name="tail",
        **params(n * 3.6e6),
    )(*args)


def solution(mesh):
    x_count = mesh.shape[ROW_AXIS]
    y_count = mesh.shape[COL_AXIS]
    vol_spec = P(PARTS_AXIS, ROW_AXIS, COL_AXIS, None)

    def swap(a, first):
        pairs = [(s, s + 1) for s in range(first, x_count - 1, 2)]
        return lax.ppermute(a, ROW_AXIS, pairs + [(b, a_) for a_, b in pairs])

    def swap_out(v):
        return [swap(v[0], 1), swap(v[1], 1)]

    def share(lo, hi):
        below = lax.ppermute(hi, COL_AXIS, [(s, s + 1) for s in range(y_count - 1)])
        above = lax.ppermute(lo, COL_AXIS, [(s + 1, s) for s in range(y_count - 1)])
        return below, above

    def local_layers(volume, filter_taps, mix_weights, mix_bias):
        n_layers = filter_taps.shape[0]
        d = Dims(volume.shape, filter_taps.shape[-1])
        h, mid = d.h, d.mid
        two = [(0, (0, 1, 2)), (1, (1, 2, 3))]
        one = [(0, (0, 1, 2))]
        flip = (lax.axis_index(ROW_AXIS) % 2).astype(jnp.int32).reshape(1)
        vol = jnp.transpose(volume, (1, 2, 3, 0))
        t_first = build_first(d, flip, filter_taps)
        lo_mid, hi_mid = direct_edges(d, t_first, vol)
        s_mid = share(lo_mid, hi_mid)
        v_in = pack(d, lo_mid, flip, vol, h + mid, h)
        h_in = [swap(v_in[0], 0)]
        v_out = pack(d, v_in[0], flip, vol, 0, h, True)
        h_out = swap_out(v_out)
        v_mid = pack(d, v_out[0], flip, vol, h, mid)
        t_in, t_mid, t_out, t_y, t_z = build_bands(d, v_mid[0], flip, filter_taps)
        w_ext = jnp.concatenate([mix_weights[:, :, :d.cm]] + [mix_weights[:, :, d.cm:]] * d.rep, axis=2)
        bias = jnp.stack([mix_bias[:, :d.cm], jnp.concatenate([mix_bias[:, d.cm:]] * d.rep, axis=1)], axis=1)
        lo_in, hi_in = xfilt_edges(d, v_mid[0], t_in[0], (v_mid, v_in, h_in))
        s_in = share(lo_in, hi_in)
        dep = lo_in
        res = None
        for layer in range(n_layers):
            first, last = layer == 0, layer == n_layers - 1
            consts = (t_y[layer], t_z[layer], w_ext[layer, :d.cm], w_ext[layer, d.cm:], bias[layer])

            def run_tail(dep, halos, lo, m, hi, v, u0, out_buf=None):
                us = (halos[0], lo, m, hi, halos[1])
                return tail(d, dep, flip, consts, us, v, last, u0, out_buf)

            if not first:
                h_out = swap_out(v_out)
                lo_mid, hi_mid = xfilt_edges(d, dep, t_mid[layer], (v_out, v_mid, v_in))
                s_mid = share(lo_mid, hi_mid)
                dep = lo_mid
            m_mid, m_in = xfilt_middle(d, dep, [t_mid[layer], t_in[layer]], (v_out, v_mid, v_in, h_in), two)
            out_trio = (h_out, v_out, v_mid)
            if first:
                w_mid = run_tail(m_mid, s_mid, lo_mid, m_mid, hi_mid, v_mid, h)
                lo_out, hi_out = xfilt_edges(d, w_mid[0], t_out[layer], out_trio)
                s_out = share(lo_out, hi_out)
                w_in = run_tail(lo_out, s_in, lo_in, m_in, hi_in, v_in, h + mid)
                h_in = [swap(w_in[0], 0)]
                (m_out,) = xfilt_middle(d, w_in[0], [t_out[layer]], out_trio, one)
            else:
                w_in = run_tail(m_mid, s_in, lo_in, m_in, hi_in, v_in, h + mid)
                if not last:
                    h_in = [swap(w_in[0], 0)]
                lo_out, hi_out = xfilt_edges(d, w_in[0], t_out[layer], out_trio)
                s_out = share(lo_out, hi_out)
                (m_out,) = xfilt_middle(d, lo_out, [t_out[layer]], out_trio, one)
                w_mid = run_tail(m_out, s_mid, lo_mid, m_mid, hi_mid, v_mid, h, w_in[0] if last else None)
            if last:
                (res,) = run_tail(m_out, s_out, lo_out, m_out, hi_out, v_out, 0, w_mid[0])
                break
            dep = m_out if first else w_mid[0]
            lo_in, hi_in = xfilt_edges(d, dep, t_in[layer + 1], (w_mid, w_in, h_in))
            s_in = share(lo_in, hi_in)
            w_out = run_tail(lo_in, s_out, lo_out, m_out, hi_out, v_out, 0)
            v_in, v_mid, v_out = w_in, w_mid, w_out
            dep = w_out[0]
        return jnp.transpose(res, (3, 0, 1, 2))

    return jax.shard_map(local_layers, mesh=mesh, in_specs=(vol_spec, P(), P(), P()), out_specs=vol_spec, check_vma=False)
```
